32 devices in a mesh: lat: 16 (over z, y, x), head: 2 (over core).
Axes of the slice: x: 2, y: 2, z: 4, core: 2. Of those that a mesh axis runs over, the one named last changes fastest.
Arguments:
- grid_latent: bfloat16 [131072, 512], P('lat'), may hold values from -6 to 6
- mesh_latent: bfloat16 [10240, 512], P('lat'), may hold values from -6 to 6
- neighbours: int32 [10240, 16], P('lat'), may hold values from -1 to 131071, as said below
- edge_bias: bfloat16 [10240, 64], P('lat', 'head'), may hold values from -8 to 384
- query_weight: bfloat16 [512, 512], P(None, 'head'), may hold values from -0.25 to 0.25
- key_weight: bfloat16 [512, 512], P(None, 'head'), may hold values from -0.25 to 0.25
- value_weight: bfloat16 [512, 512], P(None, 'head'), may hold values from -0.25 to 0.25
- out_weight: bfloat16 [512, 512], P('head'), may hold values from -0.25 to 0.25
- norm_gain: bfloat16 [512], P('head'), may hold values from 0.5 to 1.5
Outputs:
- mesh_out: bfloat16 [10240, 512], P('lat', 'head')
The draws below stay inside these ranges and needn't reach their ends.
Inputs may be any that keep to these rules, and one draw needn't show every extreme that they name: `neighbours`: every neighbour of mesh node m is -1 or lies in [b * 8192 - 2048, (b + 1) * 8192 + 2048) with b = m // 640; both ends of that range (cut to the grid) are named in every draw; slots 0 and 1 are never -1.
All inputs are finite; a program needn't handle non-finite values.
Results may differ from the reference program's by a relative error of at most 0.0075.
Values may be sent and summed in bfloat16 or wider, within the bound.
A program may use at most 128 MiB of HBM per device.

```python
import math
import jax
import jax.numpy as jnp
from jax import lax

D = 512
HEADS = 4
K = 16
G_DEV = 8192
M_DEV = 640
HEAD_DIM = 128
HALO = 2048
GRID = 131072
MESH = 10240


def draw_neighbours(key, part):
    mesh_ids = jnp.arange(MESH, dtype=jnp.int32)
    owner = mesh_ids // M_DEV
    lowest = jnp.maximum(owner * G_DEV - HALO, 0)
    highest = jnp.minimum((owner + 1) * G_DEV + HALO, GRID)
    key_pick = jax.random.fold_in(key, 11)
    key_pad = jax.random.fold_in(key, 23)
    offsets = jax.random.randint(key_pick, (MESH, K), 0, (highest - lowest)[:, None])
    picked = lowest[:, None] + offsets
    first = (mesh_ids % M_DEV == 0)[:, None]
    slot = jnp.arange(K, dtype=jnp.int32)[None, :]
    picked = jnp.where(first & (slot == 0), lowest[:, None], picked)
    picked = jnp.where(first & (slot == 1), highest[:, None] - 1, picked)
    padded = (jax.random.randint(key_pad, (MESH, K), 0, 4) == 0) & (slot >= 2)
    return jnp.where(padded, -1, picked).astype(jnp.int32)


def draw_edge_bias(key, part):
    base = jnp.clip(jax.random.normal(jax.random.fold_in(key, 37), (MESH, HEADS * K), jnp.float32), -8.0, 8.0)
    return base.astype(jnp.bfloat16)


def shard_levels(key, extent, cuts, smallest, high):
    def one(dim, shards_of):
        steps = jax.random.uniform(jax.random.fold_in(jax.random.fold_in(key, 6), dim), (shards_of,), jnp.float32, smallest / len(cuts), high / len(cuts))
        return jnp.repeat(jnp.exp(steps), extent[dim] // shards_of).reshape((-1,) + (1,) * (len(extent) - dim - 1))

    level = one(*cuts[0])
    for cut in cuts[1:]:
        level = level * one(*cut)
    return level


def gaussian(key, dims, deviation, limit, shards=(), kind=jnp.bfloat16):
    array = jax.random.normal(key, dims, jnp.float32) * deviation
    if len(shards) > 0:
        array = shard_levels(key, dims, shards, -0.22, 0.18) * array
    return jnp.clip(array, min=-limit, max=limit).astype(kind)


def setup_inputs(seed: int = 0) -> dict:
    splits = jax.random.split(jax.random.key(seed), 10)
    grid_latent = gaussian(splits[0], (GRID, D), 1.0, 6.0, ((0, 16),))
    mesh_latent = gaussian(splits[1], (MESH, D), 1.0, 6.0, ((0, 16),))
    neighbours = draw_neighbours(jax.random.fold_in(splits[9], 71), 0)
    edge_bias = draw_edge_bias(jax.random.fold_in(splits[9], 71), 0)
    query_weight = gaussian(splits[4], (D, D), D ** -0.5, 0.25, ((1, 2),))
    key_weight = gaussian(splits[5], (D, D), D ** -0.5, 0.25, ((1, 2),))
    value_weight = gaussian(splits[6], (D, D), D ** -0.5, 0.25, ((1, 2),))
    out_weight = gaussian(splits[7], (D, D), D ** -0.5, 0.25, ((0, 2),))
    norm_gain = jnp.clip(1.0 + 0.1 * jax.random.normal(splits[8], (D,), jnp.float32), 0.5, 1.5).astype(jnp.bfloat16)
    return dict(grid_latent=grid_latent, mesh_latent=mesh_latent, neighbours=neighbours, edge_bias=edge_bias, query_weight=query_weight, key_weight=key_weight, value_weight=value_weight, out_weight=out_weight, norm_gain=norm_gain)


EPSILON = 1e-05

def reference(grid_latent, mesh_latent, neighbours, edge_bias, query_weight, key_weight, value_weight, out_weight, norm_gain):

    def attend_block(blocks):
        mesh_rows, neigh_rows, bias_rows = blocks
        count = mesh_rows.shape[0]
        queries = jnp.dot(mesh_rows, query_weight, preferred_element_type=jnp.float32).astype(jnp.bfloat16)
        valid = neigh_rows >= 0
        safe_index = jnp.where(valid, neigh_rows, 0).astype(jnp.int32)
        fetched = grid_latent[safe_index.reshape(-1)]
        keys = jnp.dot(fetched, key_weight, preferred_element_type=jnp.float32).astype(jnp.bfloat16)
        values = jnp.dot(fetched, value_weight, preferred_element_type=jnp.float32).astype(jnp.bfloat16)
        keys = keys.reshape(count, K, HEADS, HEAD_DIM).astype(jnp.float32)
        values = values.reshape(count, K, HEADS, HEAD_DIM).astype(jnp.float32)
        query_heads = queries.astype(jnp.float32).reshape(count, HEADS, HEAD_DIM)
        scores = jnp.einsum('bhc,bkhc->bhk', query_heads, keys) * HEAD_DIM ** (-0.5)
        scores = scores + bias_rows.astype(jnp.float32).reshape(count, HEADS, K)
        live = valid[:, None, :]
        scores = jnp.where(live, scores, -1e+30)
        top_score = lax.optimization_barrier(jnp.max(scores, axis=2, keepdims=True))
        weights = jnp.where(live, jnp.exp(scores - top_score), 0.0)
        total = lax.optimization_barrier(jnp.sum(weights, axis=2))
        mixed = jnp.einsum('bhk,bkhc->bhc', weights, values) / total[:, :, None]
        attended = mixed.reshape(count, D).astype(jnp.bfloat16)
        projected = jnp.dot(attended, out_weight, preferred_element_type=jnp.float32)
        updated = mesh_rows.astype(jnp.float32) + projected
        mean = lax.optimization_barrier(jnp.sum(updated, axis=1)) / D
        variance = lax.optimization_barrier(jnp.sum(updated * updated, axis=1)) / D - mean * mean
        normed = (updated - mean[:, None]) * lax.rsqrt(variance[:, None] + EPSILON) * norm_gain.astype(jnp.float32)
        return normed.astype(jnp.bfloat16)
    block = math.gcd(MESH, 512)
    nblocks = MESH // block
    result = lax.map(attend_block, (mesh_latent.reshape(nblocks, block, D), neighbours.reshape(nblocks, block, K), edge_bias.reshape(nblocks, block, HEADS * K)))
    return result.reshape(MESH, D)
```

```python
import functools

import jax
import jax.numpy as jnp
from jax import lax
from jax.experimental import pallas as pl
from jax.experimental.pallas import tpu as pltpu
from jax.sharding import PartitionSpec as P

K = 16
HEAD_DIM = 128
HALO = 2048
LANES = 128
SUB = 8
NODES = LANES // K
EPSILON = 1e-05
DEAD = -1e30
PIECE = 1024
UNROLL = 4


def attend(
    order_ref,
    grid_ref,
    low_own,
    low_other,
    high_own,
    high_other,
    query_ref,
    bias_ref,
    mesh_ref,
    value_ref,
    out_weight_ref,
    gain_ref,
    out_ref,
    wide,
    picked,
    mixed,
    stage,
    sems,
):
    width = grid_ref.shape[1]
    cols = width // LANES
    band = grid_ref.shape[0]
    edges = picked.shape[0] // cols
    heads = width // HEAD_DIM
    chunk_rows = heads * NODES
    chunks = edges // LANES
    half = low_own.shape[0]
    me = lax.axis_index("head")

    pieces = []
    for start in range(0, band, PIECE):
        pieces.append((grid_ref, start, HALO + start))
    for start in range(0, half, PIECE):
        pieces.append((low_own, start, me * half + start))
        pieces.append((low_other, start, (1 - me) * half + start))
        pieces.append((high_own, start, HALO + band + me * half + start))
        pieces.append((high_other, start, HALO + band + (1 - me) * half + start))

    def fetch(n):
        ref, start, _ = pieces[n]
        return pltpu.make_async_copy(
            ref.at[pl.ds(start, PIECE)], stage.at[n % 2], sems.at[n % 2]
        )

    fetch(0).start()
    for n in range(len(pieces)):
        if n + 1 < len(pieces):
            fetch(n + 1).start()
        fetch(n).wait()
        base = pieces[n][2] * cols

        def widen(step, carry, n=n, base=base):
            for part in range(2):
                row = pl.multiple_of(step * 32 + part * 16, 16)
                block = stage[n % 2, pl.ds(row, 16), :].astype(jnp.float32)
                for t in range(2):
                    for c in range(cols):
                        at = pl.multiple_of(base + row * cols + (t * cols + c) * SUB, SUB)
                        wide[pl.ds(at, SUB), :] = block[
                            t * SUB : (t + 1) * SUB, c * LANES : (c + 1) * LANES
                        ]
            return carry

        lax.fori_loop(0, PIECE // 32, widen, 0)

    def pick(step, carry):
        for e in range(32):
            at = order_ref[step * 32 + e]
            row = wide[pl.ds(at, cols, stride=SUB), :]
            to = step * (32 * cols) + (e // SUB) * (cols * SUB) + e % SUB
            picked[pl.ds(to, cols, stride=SUB), :] = row
        return carry

    lax.fori_loop(0, edges // 32, pick, 0)

    tiles = LANES // SUB

    def score(step, carry):
        for u in range(UNROLL):
            chunk = step * UNROLL + u
            start = chunk * (LANES * cols)
            parts = []
            for c in range(cols):
                parts.append(
                    jnp.concatenate(
                        [
                            picked[
                                pl.ds(
                                    pl.multiple_of(start + (t * cols + c) * SUB, SUB), SUB
                                ),
                                :,
                            ]
                            for t in range(tiles)
                        ],
                        axis=0,
                    ).astype(jnp.bfloat16)
                )
            rows = jnp.concatenate(parts, axis=1)
            at = pl.ds(pl.multiple_of(chunk * chunk_rows, chunk_rows), chunk_rows)
            scores = lax.dot_general(
                query_ref[at, :],
                rows,
                (((1,), (1,)), ((), ())),
                preferred_element_type=jnp.float32,
            )
            scores = scores * HEAD_DIM ** (-0.5) + bias_ref[at, :]
            top = jnp.max(scores, axis=1, keepdims=True)
            weights = jnp.exp(scores - top)
            total = jnp.sum(weights, axis=1, keepdims=True)
            summed = jnp.dot(
                weights.astype(jnp.bfloat16), rows, preferred_element_type=jnp.float32
            )
            summed = summed / total
            for h in range(heads):
                mixed[h, pl.ds(pl.multiple_of(chunk * NODES, NODES), NODES), :] = summed[
                    h * NODES : (h + 1) * NODES
                ]
        return carry

    lax.fori_loop(0, chunks // UNROLL, score, 0)

    attended = jnp.concatenate(
        [
            jnp.dot(
                mixed[h].astype(jnp.bfloat16),
                value_ref[:, h * HEAD_DIM : (h + 1) * HEAD_DIM],
                preferred_element_type=jnp.float32,
            ).astype(jnp.bfloat16)
            for h in range(heads)
        ],
        axis=1,
    )
    updated = mesh_ref[...].astype(jnp.float32) + jnp.dot(
        attended, out_weight_ref[...], preferred_element_type=jnp.float32
    )
    mean = jnp.sum(updated, axis=1, keepdims=True) / width
    variance = jnp.sum(updated * updated, axis=1, keepdims=True) / width - mean * mean
    normed = (updated - mean) * lax.rsqrt(variance + EPSILON) * gain_ref[...]
    out_ref[...] = normed.astype(jnp.bfloat16)


def swap(block):
    return lax.ppermute(block, "head", [(0, 1), (1, 0)])


def ordered(own, other, me, axis):
    first = jnp.where(me == 0, own, other)
    second = jnp.where(me == 0, other, own)
    return jnp.concatenate([first, second], axis=axis)


def shards(
    grid_latent,
    mesh_latent,
    neighbours,
    edge_bias,
    query_weight,
    key_weight,
    value_weight,
    out_weight,
    norm_gain,
):
    band, width = grid_latent.shape
    count = mesh_latent.shape[0]
    part = count // 2
    cols = width // LANES
    heads = width // HEAD_DIM
    edges = part * K
    half = HALO // 2
    me = lax.axis_index("head")
    lat = lax.axis_index("lat")
    size = lax.axis_size("lat")
    forward = [(i, i + 1) for i in range(size - 1)]
    backward = [(i + 1, i) for i in range(size - 1)]
    low_own = lax.ppermute(
        lax.dynamic_slice_in_dim(grid_latent, band - HALO + me * half, half, 0), "lat", forward
    )
    high_own = lax.ppermute(
        lax.dynamic_slice_in_dim(grid_latent, me * half, half, 0), "lat", backward
    )
    low_other = swap(low_own)
    high_other = swap(high_own)

    query_all = ordered(query_weight, swap(query_weight), me, 1)
    key_all = ordered(key_weight, swap(key_weight), me, 1)
    value_all = ordered(value_weight, swap(value_weight), me, 1)
    out_all = ordered(out_weight, swap(out_weight), me, 0)
    gain_all = ordered(norm_gain, swap(norm_gain), me, 0)
    bias_own = lax.dynamic_slice_in_dim(edge_bias, me * part, part, 0)
    bias_other = swap(lax.dynamic_slice_in_dim(edge_bias, (1 - me) * part, part, 0))
    bias_all = ordered(bias_own, bias_other, me, 1)

    mesh_rows = lax.dynamic_slice_in_dim(mesh_latent, me * part, part, 0)
    neigh = lax.dynamic_slice_in_dim(neighbours, me * part, part, 0)
    valid = neigh >= 0
    local = jnp.where(valid, neigh - (lat * band - HALO), HALO)
    order = ((local // SUB) * (SUB * cols) + local % SUB).reshape(-1)

    queries = jnp.dot(mesh_rows, query_all, preferred_element_type=jnp.float32).astype(
        jnp.bfloat16
    )
    folded = jnp.einsum(
        "xnhc,dhc->xhnd",
        queries.reshape(part // NODES, NODES, heads, HEAD_DIM),
        key_all.reshape(width, heads, HEAD_DIM),
        preferred_element_type=jnp.float32,
    ).astype(jnp.bfloat16)
    folded = folded.reshape(part * heads, width)

    spread = (
        jnp.arange(K, dtype=jnp.int32)[:, None]
        == (jnp.arange(LANES, dtype=jnp.int32) % K)[None, :]
    ).astype(jnp.bfloat16)
    bias_rows = bias_all.reshape(part // NODES, NODES, heads, K).transpose(0, 2, 1, 3)
    bias_rows = jnp.dot(
        bias_rows.reshape(part * heads, K), spread, preferred_element_type=jnp.float32
    ).reshape(part // NODES, heads, NODES, LANES)
    live = jnp.dot(valid.astype(jnp.bfloat16), spread, preferred_element_type=jnp.float32)
    live = live.reshape(part // NODES, 1, NODES, LANES) > 0.5
    own_lane = (
        jnp.arange(NODES, dtype=jnp.int32)[:, None]
        == (jnp.arange(LANES, dtype=jnp.int32) // K)[None, :]
    )
    bias_rows = jnp.where(live & own_lane, bias_rows, DEAD).reshape(part * heads, LANES)

    vmem = pl.BlockSpec(memory_space=pltpu.VMEM)
    hbm = pl.BlockSpec(memory_space=pl.ANY)
    normed = pl.pallas_call(
        attend,
        name="attend",
        out_shape=jax.ShapeDtypeStruct((part, width), jnp.bfloat16),
        in_specs=[pl.BlockSpec(memory_space=pltpu.SMEM)] + [hbm] * 5 + [vmem] * 6,
        out_specs=vmem,
        scratch_shapes=[
            pltpu.VMEM(((band + 2 * HALO) * cols, LANES), jnp.float32),
            pltpu.VMEM((edges * cols, LANES), jnp.float32),
            pltpu.VMEM((heads, part, width), jnp.float32),
            pltpu.VMEM((2, PIECE, width), jnp.bfloat16),
            pltpu.SemaphoreType.DMA((2,)),
        ],
        compiler_params=pltpu.CompilerParams(vmem_limit_bytes=58 * 1024 * 1024),
    )(
        order,
        grid_latent,
        low_own,
        low_other,
        high_own,
        high_other,
        folded,
        bias_rows,
        mesh_rows,
        value_all,
        out_all,
        gain_all.astype(jnp.float32).reshape(1, width),
    )
    side = width // 2
    keep = lax.dynamic_slice_in_dim(normed, me * side, side, 1)
    give = swap(lax.dynamic_slice_in_dim(normed, (1 - me) * side, side, 1))
    return ordered(keep, give, me, 0)


def solution(mesh):
    in_specs = (
        P("lat", None),
        P("lat", None),
        P("lat", None),
        P("lat", "head"),
        P(None, "head"),
        P(None, "head"),
        P(None, "head"),
        P("head", None),
        P("head"),
    )
    out_specs = P("lat", "head")
    return jax.shard_map(shards, mesh=mesh, in_specs=in_specs, out_specs=out_specs, check_vma=False)
```

```python
import functools

import jax
import jax.numpy as jnp
from jax import lax
from jax.experimental import pallas as pl
from jax.experimental.pallas import tpu as pltpu
from jax.sharding import PartitionSpec as P

K = 16
HEAD_DIM = 128
HALO = 2048
LANES = 128
SUB = 8
NODES = LANES // K
EPSILON = 1e-05
DEAD = -1e30
PIECE = 1024
UNROLL = 4
BATCH = 16


def widen_pieces(pieces, wide, stage, sems):
    cols = stage.shape[2] // LANES

    def fetch(n):
        ref, start, _ = pieces[n]
        return pltpu.make_async_copy(
            ref.at[pl.ds(start, PIECE)], stage.at[n % 2], sems.at[n % 2]
        )

    fetch(0).start()
    for n in range(len(pieces)):
        if n + 1 < len(pieces):
            fetch(n + 1).start()
        fetch(n).wait()
        base = pieces[n][2] * cols

        def widen(step, carry, n=n, base=base):
            for part in range(2):
                row = pl.multiple_of(step * 32 + part * 16, 16)
                block = stage[n % 2, pl.ds(row, 16), :].astype(jnp.float32)
                for t in range(2):
                    for c in range(cols):
                        at = pl.multiple_of(base + row * cols + (t * cols + c) * SUB, SUB)
                        wide[pl.ds(at, SUB), :] = block[
                            t * SUB : (t + 1) * SUB, c * LANES : (c + 1) * LANES
                        ]
            return carry

        lax.fori_loop(0, PIECE // 32, widen, 0)


def collect(
    order_ref, reach_ref, grid_ref, picked_out, from_ref, to_ref, count_ref,
    wide, picked, stage, sems, out_sem,
):
    band, width = grid_ref.shape
    cols = width // LANES
    edges = order_ref.shape[0]
    widen_pieces([(grid_ref, s, s) for s in range(0, band, PIECE)], wide, stage, sems)

    def pick(step, carry):
        for e in range(32):
            at = order_ref[step * 32 + e]
            row = wide[pl.ds(at, cols, stride=SUB), :]
            to = step * (32 * cols) + (e // SUB) * (cols * SUB) + e % SUB
            picked[pl.ds(to, cols, stride=SUB), :] = row
        return carry

    lax.fori_loop(0, edges // 32, pick, 0)
    out = pltpu.make_async_copy(picked, picked_out, out_sem)
    out.start()

    def enlist(step, found):
        for e in range(16):
            far = reach_ref[step * 16 + e]
            to = step * (16 * cols) + (e // SUB) * (cols * SUB) + e % SUB
            from_ref[found] = far
            to_ref[found] = to
            found = found + jnp.where(far >= 0, 1, 0)
        return found

    found = lax.fori_loop(0, edges // 16, enlist, 0)
    for e in range(BATCH):
        from_ref[found + e] = 0
        to_ref[found + e] = edges * cols
    count_ref[0] = (found + BATCH - 1) // BATCH
    out.wait()


def attend(
    from_ref, to_ref, count_ref,
    picked_in, low_own, low_other, high_own, high_other,
    query_ref, bias_ref, mesh_ref, value_ref, out_weight_ref, gain_ref,
    out_ref,
    wide, picked, mixed, stage, sems, in_sem,
):
    width = mesh_ref.shape[1]
    cols = width // LANES
    edges = picked_in.shape[0] // cols
    heads = width // HEAD_DIM
    chunk_rows = heads * NODES
    chunks = edges // LANES
    half = low_own.shape[0]
    me = lax.axis_index("head")
    fill = pltpu.make_async_copy(picked_in, picked.at[pl.ds(0, edges * cols)], in_sem)
    fill.start()
    pieces = []
    for start in range(0, half, PIECE):
        pieces.append((low_own, start, me * half + start))
        pieces.append((high_own, start, HALO + me * half + start))
        pieces.append((low_other, start, (1 - me) * half + start))
        pieces.append((high_other, start, HALO + (1 - me) * half + start))
    widen_pieces(pieces, wide, stage, sems)
    fill.wait()

    def pick(step, carry):
        rows = []
        for e in range(BATCH):
            at = from_ref[step * BATCH + e]
            rows.append(wide[pl.ds(at, cols, stride=SUB), :])
        for e in range(BATCH):
            picked[pl.ds(to_ref[step * BATCH + e], cols, stride=SUB), :] = rows[e]
        return carry

    lax.fori_loop(0, count_ref[0], pick, 0)

    tiles = LANES // SUB

    def score(step, carry):
        for u in range(UNROLL):
            chunk = step * UNROLL + u
            start = chunk * (LANES * cols)
            parts = []
            for c in range(cols):
                parts.append(
                    jnp.concatenate(
                        [
                            picked[
                                pl.ds(
                                    pl.multiple_of(start + (t * cols + c) * SUB, SUB), SUB
                                ),
                                :,
                            ]
                            for t in range(tiles)
                        ],
                        axis=0,
                    ).astype(jnp.bfloat16)
                )
            rows = jnp.concatenate(parts, axis=1)
            at = pl.ds(pl.multiple_of(chunk * chunk_rows, chunk_rows), chunk_rows)
            scores = lax.dot_general(
                query_ref[at, :],
                rows,
                (((1,), (1,)), ((), ())),
                preferred_element_type=jnp.float32,
            )
            scores = scores * HEAD_DIM ** (-0.5) + bias_ref[at, :]
            top = jnp.max(scores, axis=1, keepdims=True)
            weights = jnp.exp(scores - top)
            total = jnp.sum(weights, axis=1, keepdims=True)
            summed = jnp.dot(
                weights.astype(jnp.bfloat16), rows, preferred_element_type=jnp.float32
            )
            summed = summed / total
            for h in range(heads):
                mixed[h, pl.ds(pl.multiple_of(chunk * NODES, NODES), NODES), :] = summed[
                    h * NODES : (h + 1) * NODES
                ]
        return carry

    lax.fori_loop(0, chunks // UNROLL, score, 0)

    attended = jnp.concatenate(
        [
            jnp.dot(
                mixed[h].astype(jnp.bfloat16),
                value_ref[:, h * HEAD_DIM : (h + 1) * HEAD_DIM],
                preferred_element_type=jnp.float32,
            ).astype(jnp.bfloat16)
            for h in range(heads)
        ],
        axis=1,
    )
    updated = mesh_ref[...].astype(jnp.float32) + jnp.dot(
        attended, out_weight_ref[...], preferred_element_type=jnp.float32
    )
    mean = jnp.sum(updated, axis=1, keepdims=True) / width
    variance = jnp.sum(updated * updated, axis=1, keepdims=True) / width - mean * mean
    normed = (updated - mean) * lax.rsqrt(variance + EPSILON) * gain_ref[...]
    out_ref[...] = normed.astype(jnp.bfloat16)


def swap(block):
    return lax.ppermute(block, "head", [(0, 1), (1, 0)])


def ordered(own, other, me, axis):
    first = jnp.where(me == 0, own, other)
    second = jnp.where(me == 0, other, own)
    return jnp.concatenate([first, second], axis=axis)


def shards(
    grid_latent,
    mesh_latent,
    neighbours,
    edge_bias,
    query_weight,
    key_weight,
    value_weight,
    out_weight,
    norm_gain,
):
    band, width = grid_latent.shape
    count = mesh_latent.shape[0]
    part = count // 2
    cols = width // LANES
    heads = width // HEAD_DIM
    edges = part * K
    half = HALO // 2
    me = lax.axis_index("head")
    lat = lax.axis_index("lat")
    size = lax.axis_size("lat")
    forward = [(i, i + 1) for i in range(size - 1)]
    backward = [(i + 1, i) for i in range(size - 1)]
    low_part = lax.dynamic_slice_in_dim(grid_latent, band - HALO + me * half, half, 0)
    high_part = lax.dynamic_slice_in_dim(grid_latent, me * half, half, 0)
    (
        low_part, high_part, mesh_latent, neighbours, edge_bias,
        query_weight, key_weight, value_weight, out_weight, norm_gain,
    ) = lax.optimization_barrier((
        low_part, high_part, mesh_latent, neighbours, edge_bias,
        query_weight, key_weight, value_weight, out_weight, norm_gain,
    ))
    low_own = lax.ppermute(low_part, "lat", forward)
    high_own = lax.ppermute(high_part, "lat", backward)
    query_all = ordered(query_weight, swap(query_weight), me, 1)
    key_all = ordered(key_weight, swap(key_weight), me, 1)
    value_all = ordered(value_weight, swap(value_weight), me, 1)
    out_all = ordered(out_weight, swap(out_weight), me, 0)
    gain_all = ordered(norm_gain, swap(norm_gain), me, 0)
    bias_own = lax.dynamic_slice_in_dim(edge_bias, me * part, part, 0)
    bias_other = swap(lax.dynamic_slice_in_dim(edge_bias, (1 - me) * part, part, 0))
    bias_all = ordered(bias_own, bias_other, me, 1)

    mesh_rows = lax.dynamic_slice_in_dim(mesh_latent, me * part, part, 0)
    neigh = lax.dynamic_slice_in_dim(neighbours, me * part, part, 0)
    valid = neigh >= 0
    local = neigh - lat * band
    near = valid & (local >= 0) & (local < band)

    def address(row):
        return (row // SUB) * (SUB * cols) + row % SUB

    order = address(jnp.where(near, local, 0)).reshape(-1)
    far = jnp.where(local < 0, local + HALO, local - band + HALO)
    reach = jnp.where(valid & ~near, address(far), -1).reshape(-1)

    queries = jnp.dot(mesh_rows, query_all, preferred_element_type=jnp.float32).astype(
        jnp.bfloat16
    )
    folded = jnp.einsum(
        "xnhc,dhc->xhnd",
        queries.reshape(part // NODES, NODES, heads, HEAD_DIM),
        key_all.reshape(width, heads, HEAD_DIM),
        preferred_element_type=jnp.float32,
    ).astype(jnp.bfloat16)
    folded = folded.reshape(part * heads, width)

    spread = (
        jnp.arange(K, dtype=jnp.int32)[:, None]
        == (jnp.arange(LANES, dtype=jnp.int32) % K)[None, :]
    ).astype(jnp.bfloat16)
    bias_rows = bias_all.reshape(part // NODES, NODES, heads, K).transpose(0, 2, 1, 3)
    bias_rows = jnp.dot(
        bias_rows.reshape(part * heads, K), spread, preferred_element_type=jnp.float32
    ).reshape(part // NODES, heads, NODES, LANES)
    live = jnp.dot(valid.astype(jnp.bfloat16), spread, preferred_element_type=jnp.float32)
    live = live.reshape(part // NODES, 1, NODES, LANES) > 0.5
    own_lane = (
        jnp.arange(NODES, dtype=jnp.int32)[:, None]
        == (jnp.arange(LANES, dtype=jnp.int32) // K)[None, :]
    )
    bias_rows = jnp.where(live & own_lane, bias_rows, DEAD).reshape(part * heads, LANES)

    vmem = pl.BlockSpec(memory_space=pltpu.VMEM)
    smem = pl.BlockSpec(memory_space=pltpu.SMEM)
    hbm = pl.BlockSpec(memory_space=pl.ANY)
    gain_row = gain_all.astype(jnp.float32).reshape(1, width)
    order, reach, folded, bias_rows, mesh_rows, value_all, out_all, gain_row = (
        lax.optimization_barrier(
            (order, reach, folded, bias_rows, mesh_rows, value_all, out_all, gain_row)
        )
    )
    picked, listed_from, listed_to, listed = pl.pallas_call(
        collect,
        name="collect",
        out_shape=(
            jax.ShapeDtypeStruct((edges * cols, LANES), jnp.float32),
            jax.ShapeDtypeStruct((edges + BATCH,), jnp.int32),
            jax.ShapeDtypeStruct((edges + BATCH,), jnp.int32),
            jax.ShapeDtypeStruct((1,), jnp.int32),
        ),
        in_specs=[smem, smem, hbm],
        out_specs=(hbm, smem, smem, smem),
        scratch_shapes=[
            pltpu.VMEM((band * cols, LANES), jnp.float32),
            pltpu.VMEM((edges * cols, LANES), jnp.float32),
            pltpu.VMEM((2, PIECE, width), jnp.bfloat16),
            pltpu.SemaphoreType.DMA((2,)),
            pltpu.SemaphoreType.DMA,
        ],
        cost_estimate=pl.CostEstimate(flops=0, bytes_accessed=100_000_000, transcendentals=0),
        compiler_params=pltpu.CompilerParams(vmem_limit_bytes=58 * 1024 * 1024),
    )(order, reach, grid_latent)
    picked, low_own, high_own = lax.optimization_barrier((picked, low_own, high_own))
    low_other = swap(low_own)
    high_other = swap(high_own)
    normed = pl.pallas_call(
        attend,
        name="attend",
        out_shape=jax.ShapeDtypeStruct((part, width), jnp.bfloat16),
        in_specs=[smem] * 3 + [hbm] * 5 + [vmem] * 6,
        out_specs=vmem,
        scratch_shapes=[
            pltpu.VMEM((2 * HALO * cols, LANES), jnp.float32),
            pltpu.VMEM((edges * cols + SUB * cols, LANES), jnp.float32),
            pltpu.VMEM((heads, part, width), jnp.float32),
            pltpu.VMEM((2, PIECE, width), jnp.bfloat16),
            pltpu.SemaphoreType.DMA((2,)),
            pltpu.SemaphoreType.DMA,
        ],
        compiler_params=pltpu.CompilerParams(vmem_limit_bytes=58 * 1024 * 1024),
    )(
        listed_from, listed_to, listed,
        picked, low_own, low_other, high_own, high_other,
        folded, bias_rows, mesh_rows, value_all, out_all, gain_row,
    )
    side = width // 2
    keep = lax.dynamic_slice_in_dim(normed, me * side, side, 1)
    give = swap(lax.dynamic_slice_in_dim(normed, (1 - me) * side, side, 1))
    return ordered(keep, give, me, 0)


def solution(mesh):
    in_specs = (
        P("lat", None),
        P("lat", None),
        P("lat", None),
        P("lat", "head"),
        P(None, "head"),
        P(None, "head"),
        P(None, "head"),
        P("head", None),
        P("head"),
    )
    out_specs = P("lat", "head")
    return jax.shard_map(shards, mesh=mesh, in_specs=in_specs, out_specs=out_specs, check_vma=False)
```

```python
import functools

import jax
import jax.numpy as jnp
from jax import lax
from jax.experimental import pallas as pl
from jax.experimental.pallas import tpu as pltpu
from jax.sharding import PartitionSpec as P

K = 16
HEAD_DIM = 128
HALO = 2048
LANES = 128
SUB = 8
NODES = LANES // K
EPSILON = 1e-05
DEAD = -1e30
PIECE = 1024
UNROLL = 8
BATCH = 16


def widen_pieces(pieces, wide, stage, sems):
    cols = stage.shape[2] // LANES

    def fetch(n):
        ref, start, _ = pieces[n]
        return pltpu.make_async_copy(
            ref.at[pl.ds(start, PIECE)], stage.at[n % 2], sems.at[n % 2]
        )

    fetch(0).start()
    for n in range(len(pieces)):
        if n + 1 < len(pieces):
            fetch(n + 1).start()
        fetch(n).wait()
        base = pieces[n][2] * cols

        def widen(step, carry, n=n, base=base):
            for part in range(2):
                row = pl.multiple_of(step * 32 + part * 16, 16)
                block = stage[n % 2, pl.ds(row, 16), :].astype(jnp.float32)
                for t in range(2):
                    for c in range(cols):
                        at = pl.multiple_of(base + row * cols + (t * cols + c) * SUB, SUB)
                        wide[pl.ds(at, SUB), :] = block[
                            t * SUB : (t + 1) * SUB, c * LANES : (c + 1) * LANES
                        ]
            return carry

        lax.fori_loop(0, PIECE // 32, widen, 0)


def collect(
    order_ref, reach_ref, grid_ref, picked_out, from_ref, to_ref, count_ref,
    wide, picked, stage, sems, out_sem,
):
    band, width = grid_ref.shape
    cols = width // LANES
    edges = order_ref.shape[0]
    widen_pieces([(grid_ref, s, s) for s in range(0, band, PIECE)], wide, stage, sems)

    def pick(step, carry):
        for e in range(32):
            at = order_ref[step * 32 + e]
            row = wide[pl.ds(at, cols, stride=SUB), :]
            to = step * (32 * cols) + (e // SUB) * (cols * SUB) + e % SUB
            picked[pl.ds(to, cols, stride=SUB), :] = row
        return carry

    lax.fori_loop(0, edges // 32, pick, 0)
    out = pltpu.make_async_copy(picked, picked_out, out_sem)
    out.start()

    def enlist(step, found):
        for e in range(16):
            far = reach_ref[step * 16 + e]
            to = step * (16 * cols) + (e // SUB) * (cols * SUB) + e % SUB
            from_ref[found] = far
            to_ref[found] = to
            found = found + jnp.where(far >= 0, 1, 0)
        return found

    found = lax.fori_loop(0, edges // 16, enlist, 0)
    for e in range(BATCH):
        from_ref[found + e] = 0
        to_ref[found + e] = edges * cols
    count_ref[0] = (found + BATCH - 1) // BATCH
    out.wait()


def attend(
    from_ref, to_ref, count_ref,
    picked_in, low_own, low_other, high_own, high_other,
    query_ref, bias_ref, mesh_ref, value_ref, out_weight_ref, gain_ref,
    out_ref,
    wide, picked, mixed, in_sem,
):
    width = mesh_ref.shape[1]
    cols = width // LANES
    edges = picked_in.shape[0] // cols
    heads = width // HEAD_DIM
    chunk_rows = heads * NODES
    chunks = edges // LANES
    half = low_own.shape[0]
    me = lax.axis_index("head")
    fill = pltpu.make_async_copy(picked_in, picked.at[pl.ds(0, edges * cols)], in_sem)
    fill.start()
    other = 1 - me
    spots = (
        (low_own, me * half),
        (high_own, HALO + me * half),
        (low_other, other * half),
        (high_other, HALO + other * half),
    )
    for ref, place in spots:
        base = place * cols

        def widen(step, carry, ref=ref, base=base):
            for part in range(2):
                row = pl.multiple_of(step * 32 + part * 16, 16)
                block = ref[pl.ds(row, 16), :].astype(jnp.float32)
                for t in range(2):
                    for c in range(cols):
                        at = pl.multiple_of(base + row * cols + (t * cols + c) * SUB, SUB)
                        wide[pl.ds(at, SUB), :] = block[
                            t * SUB : (t + 1) * SUB, c * LANES : (c + 1) * LANES
                        ]
            return carry

        lax.fori_loop(0, half // 32, widen, 0)
    fill.wait()

    def pick(step, carry):
        rows = []
        for e in range(BATCH):
            at = from_ref[step * BATCH + e]
            rows.append(wide[pl.ds(at, cols, stride=SUB), :])
        for e in range(BATCH):
            picked[pl.ds(to_ref[step * BATCH + e], cols, stride=SUB), :] = rows[e]
        return carry

    lax.fori_loop(0, count_ref[0], pick, 0)

    tiles = LANES // SUB

    def score(step, carry):
        for u in range(UNROLL):
            chunk = step * UNROLL + u
            start = chunk * (LANES * cols)
            parts = []
            for c in range(cols):
                parts.append(
                    jnp.concatenate(
                        [
                            picked[
                                pl.ds(
                                    pl.multiple_of(start + (t * cols + c) * SUB, SUB), SUB
                                ),
                                :,
                            ]
                            for t in range(tiles)
                        ],
                        axis=0,
                    ).astype(jnp.bfloat16)
                )
            rows = jnp.concatenate(parts, axis=1)
            at = pl.ds(pl.multiple_of(chunk * chunk_rows, chunk_rows), chunk_rows)
            scores = lax.dot_general(
                query_ref[at, :],
                rows,
                (((1,), (1,)), ((), ())),
                preferred_element_type=jnp.float32,
            )
            scores = scores * HEAD_DIM ** (-0.5) + bias_ref[at, :]
            top = jnp.max(scores, axis=1, keepdims=True)
            weights = jnp.exp(scores - top)
            total = jnp.sum(weights, axis=1, keepdims=True)
            summed = jnp.dot(
                weights.astype(jnp.bfloat16), rows, preferred_element_type=jnp.float32
            )
            summed = summed / total
            for h in range(heads):
                mixed[h, pl.ds(pl.multiple_of(chunk * NODES, NODES), NODES), :] = summed[
                    h * NODES : (h + 1) * NODES
                ]
        return carry

    lax.fori_loop(0, chunks // UNROLL, score, 0)

    attended = jnp.concatenate(
        [
            jnp.dot(
                mixed[h].astype(jnp.bfloat16),
                value_ref[:, h * HEAD_DIM : (h + 1) * HEAD_DIM],
                preferred_element_type=jnp.float32,
            ).astype(jnp.bfloat16)
            for h in range(heads)
        ],
        axis=1,
    )
    updated = mesh_ref[...].astype(jnp.float32) + jnp.dot(
        attended, out_weight_ref[...], preferred_element_type=jnp.float32
    )
    mean = jnp.sum(updated, axis=1, keepdims=True) / width
    variance = jnp.sum(updated * updated, axis=1, keepdims=True) / width - mean * mean
    normed = (updated - mean) * lax.rsqrt(variance + EPSILON) * gain_ref[...]
    out_ref[...] = normed.astype(jnp.bfloat16)


def swap(block):
    return lax.ppermute(block, "head", [(0, 1), (1, 0)])


def ordered(own, other, me, axis):
    first = jnp.where(me == 0, own, other)
    second = jnp.where(me == 0, other, own)
    return jnp.concatenate([first, second], axis=axis)


def shards(
    grid_latent,
    mesh_latent,
    neighbours,
    edge_bias,
    query_weight,
    key_weight,
    value_weight,
    out_weight,
    norm_gain,
):
    band, width = grid_latent.shape
    count = mesh_latent.shape[0]
    part = count // 2
    cols = width // LANES
    heads = width // HEAD_DIM
    edges = part * K
    half = HALO // 2
    me = lax.axis_index("head")
    lat = lax.axis_index("lat")
    size = lax.axis_size("lat")
    forward = [(i, i + 1) for i in range(size - 1)]
    backward = [(i + 1, i) for i in range(size - 1)]
    low_part = lax.dynamic_slice_in_dim(grid_latent, band - HALO + me * half, half, 0)
    high_part = lax.dynamic_slice_in_dim(grid_latent, me * half, half, 0)
    (
        low_part, high_part, mesh_latent, neighbours, edge_bias,
        query_weight, key_weight, value_weight, out_weight, norm_gain,
    ) = lax.optimization_barrier((
        low_part, high_part, mesh_latent, neighbours, edge_bias,
        query_weight, key_weight, value_weight, out_weight, norm_gain,
    ))
    low_own = lax.ppermute(low_part, "lat", forward)
    high_own = lax.ppermute(high_part, "lat", backward)
    query_all = ordered(query_weight, swap(query_weight), me, 1)
    key_all = ordered(key_weight, swap(key_weight), me, 1)
    value_all = ordered(value_weight, swap(value_weight), me, 1)
    out_all = ordered(out_weight, swap(out_weight), me, 0)
    gain_all = ordered(norm_gain, swap(norm_gain), me, 0)
    bias_own = lax.dynamic_slice_in_dim(edge_bias, me * part, part, 0)
    bias_other = swap(lax.dynamic_slice_in_dim(edge_bias, (1 - me) * part, part, 0))
    bias_all = ordered(bias_own, bias_other, me, 1)

    mesh_rows = lax.dynamic_slice_in_dim(mesh_latent, me * part, part, 0)
    neigh = lax.dynamic_slice_in_dim(neighbours, me * part, part, 0)
    valid = neigh >= 0
    local = neigh - lat * band
    near = valid & (local >= 0) & (local < band)

    def address(row):
        return (row // SUB) * (SUB * cols) + row % SUB

    order = address(jnp.where(near, local, 0)).reshape(-1)
    beyond = jnp.where(local < 0, local + HALO, local - band + HALO)
    reach = jnp.where(valid & ~near, address(beyond), -1).reshape(-1)

    queries = jnp.dot(mesh_rows, query_all, preferred_element_type=jnp.float32).astype(
        jnp.bfloat16
    )
    folded = jnp.einsum(
        "xnhc,dhc->xhnd",
        queries.reshape(part // NODES, NODES, heads, HEAD_DIM),
        key_all.reshape(width, heads, HEAD_DIM),
        preferred_element_type=jnp.float32,
    ).astype(jnp.bfloat16)
    folded = folded.reshape(part * heads, width)

    spread = (
        jnp.arange(K, dtype=jnp.int32)[:, None]
        == (jnp.arange(LANES, dtype=jnp.int32) % K)[None, :]
    ).astype(jnp.bfloat16)
    bias_rows = bias_all.reshape(part // NODES, NODES, heads, K).transpose(0, 2, 1, 3)
    bias_rows = jnp.dot(
        bias_rows.reshape(part * heads, K), spread, preferred_element_type=jnp.float32
    ).reshape(part // NODES, heads, NODES, LANES)
    live = jnp.dot(valid.astype(jnp.bfloat16), spread, preferred_element_type=jnp.float32)
    live = live.reshape(part // NODES, 1, NODES, LANES) > 0.5
    own_lane = (
        jnp.arange(NODES, dtype=jnp.int32)[:, None]
        == (jnp.arange(LANES, dtype=jnp.int32) // K)[None, :]
    )
    bias_rows = jnp.where(live & own_lane, bias_rows, DEAD).reshape(part * heads, LANES)

    vmem = pl.BlockSpec(memory_space=pltpu.VMEM)
    smem = pl.BlockSpec(memory_space=pltpu.SMEM)
    far = pl.BlockSpec(memory_space=pltpu.HBM)
    gain_row = gain_all.astype(jnp.float32).reshape(1, width)
    picked, listed_from, listed_to, listed = pl.pallas_call(
        collect,
        name="collect",
        out_shape=(
            jax.ShapeDtypeStruct((edges * cols, LANES), jnp.float32),
            jax.ShapeDtypeStruct((edges + BATCH,), jnp.int32),
            jax.ShapeDtypeStruct((edges + BATCH,), jnp.int32),
            jax.ShapeDtypeStruct((1,), jnp.int32),
        ),
        in_specs=[smem, smem, far],
        out_specs=(far, smem, smem, smem),
        scratch_shapes=[
            pltpu.VMEM((band * cols, LANES), jnp.float32),
            pltpu.VMEM((edges * cols, LANES), jnp.float32),
            pltpu.VMEM((2, PIECE, width), jnp.bfloat16),
            pltpu.SemaphoreType.DMA((2,)),
            pltpu.SemaphoreType.DMA,
        ],
        cost_estimate=pl.CostEstimate(flops=0, bytes_accessed=100_000_000, transcendentals=0),
        compiler_params=pltpu.CompilerParams(vmem_limit_bytes=40 * 1024 * 1024),
    )(order, reach, grid_latent)
    picked, low_own, high_own, folded, bias_rows, mesh_rows, value_all, out_all, gain_row = (
        lax.optimization_barrier((
            picked, low_own, high_own,
            folded, bias_rows, mesh_rows, value_all, out_all, gain_row,
        ))
    )
    low_other = swap(low_own)
    high_other = swap(high_own)
    normed = pl.pallas_call(
        attend,
        name="attend",
        out_shape=jax.ShapeDtypeStruct((part, width), jnp.bfloat16),
        in_specs=[smem] * 3 + [far] + [vmem] * 10,
        out_specs=vmem,
        scratch_shapes=[
            pltpu.VMEM((2 * HALO * cols, LANES), jnp.float32),
            pltpu.VMEM((edges * cols + SUB * cols, LANES), jnp.float32),
            pltpu.VMEM((heads, part, width), jnp.float32),
            pltpu.SemaphoreType.DMA,
        ],
        compiler_params=pltpu.CompilerParams(vmem_limit_bytes=40 * 1024 * 1024),
    )(
        listed_from, listed_to, listed,
        picked, low_own, low_other, high_own, high_other,
        folded, bias_rows, mesh_rows, value_all, out_all, gain_row,
    )
    side = width // 2
    keep = lax.dynamic_slice_in_dim(normed, me * side, side, 1)
    give = swap(lax.dynamic_slice_in_dim(normed, (1 - me) * side, side, 1))
    return ordered(keep, give, me, 0)


def solution(mesh):
    in_specs = (
        P("lat", None),
        P("lat", None),
        P("lat", None),
        P("lat", "head"),
        P(None, "head"),
        P(None, "head"),
        P(None, "head"),
        P("head", None),
        P("head"),
    )
    out_specs = P("lat", "head")
    return jax.shard_map(shards, mesh=mesh, in_specs=in_specs, out_specs=out_specs, check_vma=False)
```

```python
import functools

import jax
import jax.numpy as jnp
from jax import lax
from jax.experimental import pallas as pl
from jax.experimental.pallas import tpu as pltpu
from jax.sharding import PartitionSpec as P

K = 16
HEAD_DIM = 128
HALO = 2048
LANES = 128
SUB = 8
NODES = LANES // K
EPSILON = 1e-05
DEAD = -1e30
PIECE = 1024
UNROLL = 8
BATCH = 16


def widen_pieces(pieces, wide, stage, sems):
    cols = stage.shape[2] // LANES

    def fetch(n):
        ref, start, _ = pieces[n]
        return pltpu.make_async_copy(
            ref.at[pl.ds(start, PIECE)], stage.at[n % 2], sems.at[n % 2]
        )

    fetch(0).start()
    for n in range(len(pieces)):
        if n + 1 < len(pieces):
            fetch(n + 1).start()
        fetch(n).wait()
        base = pieces[n][2] * cols

        def widen(step, carry, n=n, base=base):
            for part in range(2):
                row = pl.multiple_of(step * 32 + part * 16, 16)
                block = stage[n % 2, pl.ds(row, 16), :].astype(jnp.float32)
                for t in range(2):
                    for c in range(cols):
                        at = pl.multiple_of(base + row * cols + (t * cols + c) * SUB, SUB)
                        wide[pl.ds(at, SUB), :] = block[
                            t * SUB : (t + 1) * SUB, c * LANES : (c + 1) * LANES
                        ]
            return carry

        lax.fori_loop(0, PIECE // 32, widen, 0)


def collect(
    order_ref, reach_ref, grid_ref, picked_out, from_ref, to_ref, count_ref,
    wide, picked, stage, sems, out_sem,
):
    band, width = grid_ref.shape
    cols = width // LANES
    edges = order_ref.shape[0]
    widen_pieces([(grid_ref, s, s) for s in range(0, band, PIECE)], wide, stage, sems)

    def pick(step, carry):
        for e in range(32):
            at = order_ref[step * 32 + e]
            row = wide[pl.ds(at, cols, stride=SUB), :]
            to = step * (32 * cols) + (e // SUB) * (cols * SUB) + e % SUB
            picked[pl.ds(to, cols, stride=SUB), :] = row
        return carry

    lax.fori_loop(0, edges // 32, pick, 0)
    out = pltpu.make_async_copy(picked, picked_out, out_sem)
    out.start()

    def enlist(step, found):
        for e in range(16):
            far = reach_ref[step * 16 + e]
            to = step * (16 * cols) + (e // SUB) * (cols * SUB) + e % SUB
            from_ref[found] = far
            to_ref[found] = to
            found = found + jnp.where(far >= 0, 1, 0)
        return found

    found = lax.fori_loop(0, edges // 16, enlist, 0)
    for e in range(BATCH):
        from_ref[found + e] = 0
        to_ref[found + e] = edges * cols
    count_ref[0] = (found + BATCH - 1) // BATCH
    out.wait()


def attend(
    from_ref, to_ref, count_ref,
    picked_in, low_own, low_other, high_own, high_other,
    query_ref, bias_ref, mesh_in, value_in, out_weight_in, gain_ref,
    out_ref,
    wide, picked, mixed, mesh_ref, value_ref, out_weight_ref, in_sem, late_sems,
):
    width = mesh_ref.shape[1]
    cols = width // LANES
    edges = picked_in.shape[0] // cols
    heads = width // HEAD_DIM
    chunk_rows = heads * NODES
    chunks = edges // LANES
    half = low_own.shape[0]
    me = lax.axis_index("head")
    fill = pltpu.make_async_copy(picked_in, picked.at[pl.ds(0, edges * cols)], in_sem)
    fill.start()
    late = [
        pltpu.make_async_copy(mesh_in, mesh_ref, late_sems.at[0]),
        pltpu.make_async_copy(value_in, value_ref, late_sems.at[1]),
        pltpu.make_async_copy(out_weight_in, out_weight_ref, late_sems.at[2]),
    ]
    for copy in late:
        copy.start()
    other = 1 - me
    spots = (
        (low_own, me * half),
        (high_own, HALO + me * half),
        (low_other, other * half),
        (high_other, HALO + other * half),
    )
    for ref, place in spots:
        base = place * cols

        def widen(step, carry, ref=ref, base=base):
            for part in range(2):
                row = pl.multiple_of(step * 32 + part * 16, 16)
                block = ref[pl.ds(row, 16), :].astype(jnp.float32)
                for t in range(2):
                    for c in range(cols):
                        at = pl.multiple_of(base + row * cols + (t * cols + c) * SUB, SUB)
                        wide[pl.ds(at, SUB), :] = block[
                            t * SUB : (t + 1) * SUB, c * LANES : (c + 1) * LANES
                        ]
            return carry

        lax.fori_loop(0, half // 32, widen, 0)
    fill.wait()

    def pick(step, carry):
        rows = []
        for e in range(BATCH):
            at = from_ref[step * BATCH + e]
            rows.append(wide[pl.ds(at, cols, stride=SUB), :])
        for e in range(BATCH):
            picked[pl.ds(to_ref[step * BATCH + e], cols, stride=SUB), :] = rows[e]
        return carry

    lax.fori_loop(0, count_ref[0], pick, 0)

    tiles = LANES // SUB

    def score(step, carry):
        for u in range(UNROLL):
            chunk = step * UNROLL + u
            start = chunk * (LANES * cols)
            parts = []
            for c in range(cols):
                parts.append(
                    jnp.concatenate(
                        [
                            picked[
                                pl.ds(
                                    pl.multiple_of(start + (t * cols + c) * SUB, SUB), SUB
                                ),
                                :,
                            ]
                            for t in range(tiles)
                        ],
                        axis=0,
                    ).astype(jnp.bfloat16)
                )
            rows = jnp.concatenate(parts, axis=1)
            at = pl.ds(pl.multiple_of(chunk * chunk_rows, chunk_rows), chunk_rows)
            scores = lax.dot_general(
                query_ref[at, :],
                rows,
                (((1,), (1,)), ((), ())),
                preferred_element_type=jnp.float32,
            )
            scores = scores * HEAD_DIM ** (-0.5) + bias_ref[at, :]
            top = jnp.max(scores, axis=1, keepdims=True)
            weights = jnp.exp(scores - top)
            total = jnp.sum(weights, axis=1, keepdims=True)
            summed = jnp.dot(
                weights.astype(jnp.bfloat16), rows, preferred_element_type=jnp.float32
            )
            summed = summed / total
            for h in range(heads):
                mixed[h, pl.ds(pl.multiple_of(chunk * NODES, NODES), NODES), :] = summed[
                    h * NODES : (h + 1) * NODES
                ]
        return carry

    lax.fori_loop(0, chunks // UNROLL, score, 0)

    for copy in late:
        copy.wait()
    attended = jnp.concatenate(
        [
            jnp.dot(
                mixed[h].astype(jnp.bfloat16),
                value_ref[:, h * HEAD_DIM : (h + 1) * HEAD_DIM],
                preferred_element_type=jnp.float32,
            ).astype(jnp.bfloat16)
            for h in range(heads)
        ],
        axis=1,
    )
    updated = mesh_ref[...].astype(jnp.float32) + jnp.dot(
        attended, out_weight_ref[...], preferred_element_type=jnp.float32
    )
    mean = jnp.sum(updated, axis=1, keepdims=True) / width
    variance = jnp.sum(updated * updated, axis=1, keepdims=True) / width - mean * mean
    normed = (updated - mean) * lax.rsqrt(variance + EPSILON) * gain_ref[...]
    out_ref[...] = normed.astype(jnp.bfloat16)


def swap(block):
    return lax.ppermute(block, "head", [(0, 1), (1, 0)])


def ordered(own, other, me, axis):
    first = jnp.where(me == 0, own, other)
    second = jnp.where(me == 0, other, own)
    return jnp.concatenate([first, second], axis=axis)


def shards(
    grid_latent,
    mesh_latent,
    neighbours,
    edge_bias,
    query_weight,
    key_weight,
    value_weight,
    out_weight,
    norm_gain,
):
    band, width = grid_latent.shape
    count = mesh_latent.shape[0]
    part = count // 2
    cols = width // LANES
    heads = width // HEAD_DIM
    edges = part * K
    half = HALO // 2
    me = lax.axis_index("head")
    lat = lax.axis_index("lat")
    size = lax.axis_size("lat")
    forward = [(i, i + 1) for i in range(size - 1)]
    backward = [(i + 1, i) for i in range(size - 1)]
    low_part = lax.dynamic_slice_in_dim(grid_latent, band - HALO + me * half, half, 0)
    high_part = lax.dynamic_slice_in_dim(grid_latent, me * half, half, 0)
    (
        low_part, high_part, mesh_latent, neighbours, edge_bias,
        query_weight, key_weight, value_weight, out_weight, norm_gain,
    ) = lax.optimization_barrier((
        low_part, high_part, mesh_latent, neighbours, edge_bias,
        query_weight, key_weight, value_weight, out_weight, norm_gain,
    ))
    low_own = lax.ppermute(low_part, "lat", forward)
    high_own = lax.ppermute(high_part, "lat", backward)
    query_all = ordered(query_weight, swap(query_weight), me, 1)
    key_all = ordered(key_weight, swap(key_weight), me, 1)
    value_all = ordered(value_weight, swap(value_weight), me, 1)
    out_all = ordered(out_weight, swap(out_weight), me, 0)
    gain_all = ordered(norm_gain, swap(norm_gain), me, 0)
    bias_own = lax.dynamic_slice_in_dim(edge_bias, me * part, part, 0)
    bias_other = swap(lax.dynamic_slice_in_dim(edge_bias, (1 - me) * part, part, 0))
    bias_all = ordered(bias_own, bias_other, me, 1)

    mesh_rows = lax.dynamic_slice_in_dim(mesh_latent, me * part, part, 0)
    neigh = lax.dynamic_slice_in_dim(neighbours, me * part, part, 0)
    valid = neigh >= 0
    local = neigh - lat * band
    near = valid & (local >= 0) & (local < band)

    def address(row):
        return (row // SUB) * (SUB * cols) + row % SUB

    order = address(jnp.where(near, local, 0)).reshape(-1)
    beyond = jnp.where(local < 0, local + HALO, local - band + HALO)
    reach = jnp.where(valid & ~near, address(beyond), -1).reshape(-1)

    queries = jnp.dot(mesh_rows, query_all, preferred_element_type=jnp.float32).astype(
        jnp.bfloat16
    )
    folded = jnp.einsum(
        "xnhc,dhc->xhnd",
        queries.reshape(part // NODES, NODES, heads, HEAD_DIM),
        key_all.reshape(width, heads, HEAD_DIM),
        preferred_element_type=jnp.float32,
    ).astype(jnp.bfloat16)
    folded = folded.reshape(part * heads, width)

    spread = (
        jnp.arange(K, dtype=jnp.int32)[:, None]
        == (jnp.arange(LANES, dtype=jnp.int32) % K)[None, :]
    ).astype(jnp.bfloat16)
    bias_rows = bias_all.reshape(part // NODES, NODES, heads, K).transpose(0, 2, 1, 3)
    bias_rows = jnp.dot(
        bias_rows.reshape(part * heads, K), spread, preferred_element_type=jnp.float32
    ).reshape(part // NODES, heads, NODES, LANES)
    live = jnp.dot(valid.astype(jnp.bfloat16), spread, preferred_element_type=jnp.float32)
    live = live.reshape(part // NODES, 1, NODES, LANES) > 0.5
    own_lane = (
        jnp.arange(NODES, dtype=jnp.int32)[:, None]
        == (jnp.arange(LANES, dtype=jnp.int32) // K)[None, :]
    )
    bias_rows = jnp.where(live & own_lane, bias_rows, DEAD).reshape(part * heads, LANES)

    vmem = pl.BlockSpec(memory_space=pltpu.VMEM)
    smem = pl.BlockSpec(memory_space=pltpu.SMEM)
    far = pl.BlockSpec(memory_space=pltpu.HBM)
    gain_row = gain_all.astype(jnp.float32).reshape(1, width)
    picked, listed_from, listed_to, listed = pl.pallas_call(
        collect,
        name="collect",
        out_shape=(
            jax.ShapeDtypeStruct((edges * cols, LANES), jnp.float32),
            jax.ShapeDtypeStruct((edges + BATCH,), jnp.int32),
            jax.ShapeDtypeStruct((edges + BATCH,), jnp.int32),
            jax.ShapeDtypeStruct((1,), jnp.int32),
        ),
        in_specs=[smem, smem, far],
        out_specs=(far, smem, smem, smem),
        scratch_shapes=[
            pltpu.VMEM((band * cols, LANES), jnp.float32),
            pltpu.VMEM((edges * cols, LANES), jnp.float32),
            pltpu.VMEM((2, PIECE, width), jnp.bfloat16),
            pltpu.SemaphoreType.DMA((2,)),
            pltpu.SemaphoreType.DMA,
        ],
        cost_estimate=pl.CostEstimate(flops=0, bytes_accessed=100_000_000, transcendentals=0),
        compiler_params=pltpu.CompilerParams(vmem_limit_bytes=40 * 1024 * 1024),
    )(order, reach, grid_latent)
    picked, low_own, high_own, folded, bias_rows, mesh_rows, value_all, out_all, gain_row = (
        lax.optimization_barrier((
            picked, low_own, high_own,
            folded, bias_rows, mesh_rows, value_all, out_all, gain_row,
        ))
    )
    low_other = swap(low_own)
    high_other = swap(high_own)
    normed = pl.pallas_call(
        attend,
        name="attend",
        out_shape=jax.ShapeDtypeStruct((part, width), jnp.bfloat16),
        in_specs=[smem] * 3 + [far] + [vmem] * 6 + [far] * 3 + [vmem],
        out_specs=vmem,
        scratch_shapes=[
            pltpu.VMEM((2 * HALO * cols, LANES), jnp.float32),
            pltpu.VMEM((edges * cols + SUB * cols, LANES), jnp.float32),
            pltpu.VMEM((heads, part, width), jnp.float32),
            pltpu.VMEM((part, width), jnp.bfloat16),
            pltpu.VMEM((width, width), jnp.bfloat16),
            pltpu.VMEM((width, width), jnp.bfloat16),
            pltpu.SemaphoreType.DMA,
            pltpu.SemaphoreType.DMA((3,)),
        ],
        compiler_params=pltpu.CompilerParams(vmem_limit_bytes=40 * 1024 * 1024),
    )(
        listed_from, listed_to, listed,
        picked, low_own, low_other, high_own, high_other,
        folded, bias_rows, mesh_rows, value_all, out_all, gain_row,
    )
    side = width // 2
    keep = lax.dynamic_slice_in_dim(normed, me * side, side, 1)
    give = swap(lax.dynamic_slice_in_dim(normed, (1 - me) * side, side, 1))
    return ordered(keep, give, me, 0)


def solution(mesh):
    in_specs = (
        P("lat", None),
        P("lat", None),
        P("lat", None),
        P("lat", "head"),
        P(None, "head"),
        P(None, "head"),
        P(None, "head"),
        P("head", None),
        P("head"),
    )
    out_specs = P("lat", "head")
    return jax.shard_map(shards, mesh=mesh, in_specs=in_specs, out_specs=out_specs, check_vma=False)
```
